32 devices in a mesh: seq: 8 (over z, core), vocab: 4 (over y, x).
Axes of the slice: x: 2, y: 2, z: 4, core: 2. Of those that a mesh axis runs over, the one named last changes fastest.
Arguments:
- token_ids: int32 [1024], P('seq'), may hold values from 0 to 76031, as said below
- routes: int32 [256, 1], P('seq'), may hold values from 0 to 7; in each aligned block of 32 rows (0 to 31, 32 to 63, ...) at most 8 rows name the same one
- splice_start: int32 [8], P('seq'), may hold values from 0 to 64
- vision: bfloat16 [256, 5120], P('seq'), may hold values from -6 to 6
- ln_gain: float32 [1280], replicated, may hold values from 0.25 to 1.75
- table: bfloat16 [76032, 8192], P('seq', 'vocab'), may hold values from -6 to 6
- w_fc1: bfloat16 [5120, 5120], P('seq', 'vocab'), may hold values from -0.078125 to 0.078125
- w_fc2: bfloat16 [5120, 8192], P('seq', 'vocab'), may hold values from -0.078125 to 0.078125
Outputs:
- embedded: bfloat16 [1024, 8192], P('seq', 'vocab')
The draws below stay inside these ranges and needn't reach their ends.
Inputs may be any that keep to these rules, and one draw needn't show every extreme that they name: `routes`: among the rows of one shard of 32 rows no sequence is named by more than 8 rows. `token_ids`: split the vocabulary into 8 equal ranges of consecutive ids; within one sequence of 128 tokens at most 32 ids fall in one range, and every sequence has a range with exactly 32.
All inputs are finite; a program needn't handle non-finite values.
Results may differ from the reference program's by a relative error of at most 0.0055.
Values may be sent and summed in bfloat16 or wider, within the bound.
A program may use at most 128 MiB of HBM per device.

```python
import math
import jax
import jax.numpy as jnp
import numpy as np
from jax import lax

D = 8192
VIS = 1280
VOCAB = 76032
TOK_OWN = 128
MERGE = 5120
SLOTS = 32
PAIR_CAP = 8
ROWS_ALL = 256
N_SEQ = 8


def draw_token_ids(key, part):
    id_cap = 2 * TOK_OWN // N_SEQ
    shard_rows = VOCAB // N_SEQ
    half = TOK_OWN // 2
    heavy = 3 * id_cap // 4

    def one_sequence(seq_key):
        key_hot, key_order, key_offset = jax.random.split(seq_key, 3)
        hot = jax.random.randint(key_hot, (), 0, N_SEQ).astype(jnp.int32)
        places = jnp.arange(TOK_OWN, dtype=jnp.int32)
        others = places - half - heavy
        second = jnp.where(places - half < heavy, hot, (hot + 1 + others % (N_SEQ - 1)) % N_SEQ)
        labels = jnp.where(places < half, places % N_SEQ, second).astype(jnp.int32)
        labels = jax.random.permutation(key_order, labels)
        offsets = jax.random.randint(key_offset, (TOK_OWN,), 0, shard_rows).astype(jnp.int32)
        return (labels * shard_rows + offsets).astype(jnp.int32)
    keys = jax.random.split(jax.random.fold_in(key, 7), N_SEQ)
    return jax.vmap(one_sequence)(keys).reshape(N_SEQ * TOK_OWN).astype(jnp.int32)


def with_ends(array, rng, smallest, largest):
    place = [jax.random.randint(jax.random.fold_in(rng, axis), (), 0, length) for axis, length in enumerate(array.shape)]
    longest = array.shape.index(max(array.shape))
    beside = place[:longest] + [(place[longest] + 1) % array.shape[longest]] + place[longest + 1:]
    return array.at[tuple(place)].set(smallest).at[tuple(beside)].set(largest)


def block_scale(stream_key, dims, cuts, low, high):
    def one(dim, blocks):
        heights = jax.random.uniform(jax.random.fold_in(jax.random.fold_in(stream_key, 6), dim), (blocks,), jnp.float32, low / len(cuts), high / len(cuts))
        return jnp.repeat(jnp.exp(heights), dims[dim] // blocks).reshape((-1,) + (1,) * (len(dims) - dim - 1))

    level = one(*cuts[0])
    for cut in cuts[1:]:
        level = level * one(*cut)
    return level


def shared_out(own_key, own, number, rows, count, top, most, lean):
    sequence = jax.random.permutation(own_key, count)
    heavy_load, ordinary = portions_of(count, rows * top, most, lean, True), portions_of(count, rows * top, most, lean, False)
    places = jnp.arange(count)

    def named(sizes, offset_by):
        used = int((sizes > 0).sum())
        fixed = max(1, used // 4)
        shifted = fixed + (places - fixed + offset_by * (used - fixed)) % max(1, count - fixed)
        return jnp.zeros((count,), jnp.int32).at[sequence[jnp.where(places < fixed, places, shifted)]].set(jnp.asarray(sizes, jnp.int32))

    sizes = jnp.where(number % 4 == 0, named(heavy_load, number // 4), named(ordinary, number - number // 4 - 1))
    mixed = jax.random.permutation(jax.random.fold_in(own, 3), count)
    source_of, receiver = mixed[0:count // 2 * 2:2], mixed[1:count // 2 * 2:2]
    margin = jnp.minimum(sizes[source_of] - 1, most - sizes[receiver]) // 2
    margin = jnp.where((source_of == sequence[0]) | (receiver == sequence[0]) | (sizes[receiver] == 0), 0, jnp.maximum(margin, 0))
    shifted = jax.random.randint(jax.random.fold_in(own, 4), (count // 2,), 0, 1 << 20) % (margin + 1)
    sizes = sizes.at[source_of].add(-shifted).at[receiver].add(shifted)
    items = jnp.searchsorted(jnp.cumsum(sizes), jnp.arange(rows * top), side="right").astype(jnp.int32)
    table = items.reshape(top, rows).T
    table = table[jax.random.permutation(jax.random.fold_in(own, 1), rows)]
    offset_by = jax.random.randint(jax.random.fold_in(own, 2), (rows, 1), 0, top)
    return jnp.take_along_axis(table, (jnp.arange(top)[None, :] + offset_by) % top, axis=1)


def portions_of(number_of, total, most, skew, full):
    weights = [(1 << 20) // math.isqrt(grade ** skew) + 1 for grade in range(1, number_of + 1)]
    largest = most if full else min(most, max(-(-total // number_of), total * weights[0] // sum(weights)))
    least = 1 if total - largest >= number_of - 1 else 0
    counts, rest = [largest] + [least] * (number_of - 1), total - largest - least * (number_of - 1)
    while rest > 0:
        movable = [i for i in range(1, number_of) if counts[i] < largest] or [i for i in range(1, number_of) if counts[i] < most]
        pool, left = sum([weights[i] for i in movable]), rest
        for i in movable:
            addition = min(most - counts[i], max(1, left * weights[i] // pool), rest)
            counts[i] = counts[i] + addition
            rest = rest - addition
    return np.array(counts)


def noise(key, dims, width, bound, shards=(), held_as=jnp.bfloat16):
    array = width * jax.random.normal(key, dims, jnp.float32)
    if shards:
        array = array * block_scale(key, dims, shards, -0.22, 0.18)
    return jnp.clip(array, -bound, bound).astype(held_as)


def setup_inputs(seed: int = 0) -> dict:
    seeds = jax.random.split(jax.random.key(seed), 9)
    token_ids = draw_token_ids(jax.random.fold_in(seeds[8], 71), 0)
    routes_keys = jax.random.split(jax.random.fold_in(seeds[1], 1), ROWS_ALL // SLOTS)
    routes_turns = jax.random.permutation(jax.random.fold_in(seeds[1], 3), ROWS_ALL // SLOTS)
    routes = jax.vmap(lambda own, number: shared_out(jax.random.fold_in(seeds[1], 2), own, number, SLOTS, N_SEQ, 1, PAIR_CAP, 2))(routes_keys, routes_turns).reshape((ROWS_ALL, 1))
    splice_start = with_ends(jax.random.randint(seeds[2], (N_SEQ,), 0, TOK_OWN - 2 * SLOTS + 1), jax.random.fold_in(seeds[2], 1), 0, TOK_OWN - 2 * SLOTS).astype(jnp.int32)
    vision = noise(seeds[3], (ROWS_ALL, MERGE), 1.0, 6.0, ((0, 8),))
    ln_gain = jnp.clip(1.0 + 0.15 * jax.random.normal(seeds[4], (VIS,), jnp.float32), 0.25, 1.75)
    table = noise(seeds[5], (VOCAB, D), 1.0, 6.0, ((0, 8), (1, 4)))
    w_fc1 = noise(seeds[6], (MERGE, MERGE), MERGE ** -0.5, 0.078125, ((0, 8), (1, 4)))
    w_fc2 = noise(seeds[7], (MERGE, D), MERGE ** -0.5, 0.078125, ((0, 8), (1, 4)))
    return dict(token_ids=token_ids, routes=routes, splice_start=splice_start, vision=vision, ln_gain=ln_gain, table=table, w_fc1=w_fc1, w_fc2=w_fc2)


def layer_norm(vision, ln_gain):
    rows = vision.shape[0]
    values = vision.astype(jnp.float32).reshape(rows, 4, ln_gain.shape[0])
    center = values - lax.optimization_barrier(jnp.mean(values, axis=-1, keepdims=True))
    spread = lax.optimization_barrier(jnp.mean(center * center, axis=-1, keepdims=True))
    normed = center / jnp.sqrt(spread + 1e-06) * ln_gain.astype(jnp.float32)
    return normed.reshape(rows, 4 * ln_gain.shape[0]).astype(jnp.bfloat16)

def reference(token_ids, routes, splice_start, vision, ln_gain, table, w_fc1, w_fc2):
    text = jnp.take(table, token_ids.astype(jnp.int32), axis=0)
    normed = layer_norm(vision, ln_gain)
    pre = jnp.dot(normed, w_fc1, preferred_element_type=jnp.float32)
    hidden = jax.nn.gelu(pre, approximate=False).astype(jnp.bfloat16)
    merged = jnp.dot(hidden, w_fc2, preferred_element_type=jnp.float32).astype(jnp.bfloat16)
    owners = routes[:, 0].astype(jnp.int32)
    owner_hot = (owners[:, None] == jnp.arange(N_SEQ, dtype=jnp.int32)[None, :]).astype(jnp.int32)
    earlier = jnp.cumsum(owner_hot, axis=0) - owner_hot
    rank = lax.optimization_barrier(jnp.sum(earlier * owner_hot, axis=1)).astype(jnp.int32)
    target = (owners * TOK_OWN + jnp.take(splice_start, owners).astype(jnp.int32) + rank).astype(jnp.int32)
    return text.at[target].set(merged)
```

```python
import math

import jax
import jax.numpy as jnp
from jax import lax
from jax.experimental import pallas as pl
from jax.experimental.pallas import tpu as pltpu
from jax.sharding import PartitionSpec as P


TILE = 8


def gather_kernel(ids_ref, pick_ref, table_ref, out_ref, held, sems):
    groups, cap, _ = out_ref.shape

    def issue(g, carry):
        def one(k, c):
            row = pl.multiple_of(ids_ref[g, k] // TILE * TILE, TILE)
            at = pl.multiple_of((g * cap + k) * TILE, TILE)
            pltpu.make_async_copy(
                table_ref.at[pl.ds(row, TILE), :], held.at[pl.ds(at, TILE), :], sems.at[g]
            ).start()
            return c

        return lax.fori_loop(0, cap, one, carry)

    lax.fori_loop(0, groups, issue, 0)

    def finish(g, carry):
        at = pl.multiple_of(g * cap * TILE, TILE)
        block = held.at[pl.ds(at, cap * TILE), :]
        pltpu.make_async_copy(block, block, sems.at[g]).wait()
        out_ref[g] = jnp.dot(
            pick_ref[g], block[...], preferred_element_type=jnp.float32
        ).astype(out_ref.dtype)
        return carry

    lax.fori_loop(0, groups, finish, 0)


def gather_rows(local_ids, table):
    groups, cap = local_ids.shape
    width = table.shape[1]
    lane = jnp.arange(cap * TILE, dtype=jnp.int32)
    slot = jnp.arange(cap, dtype=jnp.int32)[None, :] * TILE + local_ids % TILE
    pick = (slot[:, :, None] == lane[None, None, :]).astype(jnp.bfloat16)
    return pl.pallas_call(
        gather_kernel,
        out_shape=jax.ShapeDtypeStruct((groups, cap, width), table.dtype),
        in_specs=[
            pl.BlockSpec(memory_space=pltpu.SMEM),
            pl.BlockSpec(memory_space=pltpu.VMEM),
            pl.BlockSpec(memory_space=pl.ANY),
        ],
        out_specs=pl.BlockSpec(memory_space=pltpu.VMEM),
        scratch_shapes=[
            pltpu.VMEM((groups * cap * TILE, width), table.dtype),
            pltpu.SemaphoreType.DMA((groups,)),
        ],
        name="gather_rows",
    )(local_ids, pick, table)


def route_plan(token_ids, routes, splice_start, shard_rows):
    seq_count = lax.axis_size("seq")
    seq_index = lax.axis_index("seq")
    local_rows = token_ids.shape[0]
    slot_rows = routes.shape[0]
    pair_cap = 2 * slot_rows // seq_count
    id_cap = 2 * local_rows // seq_count
    both = lax.all_gather(jnp.concatenate([token_ids, routes[:, 0]]), "seq", axis=0)
    all_ids, all_routes = both[:, :local_rows], both[:, local_rows:]
    mine = all_ids // shard_rows == seq_index
    place = jnp.cumsum(mine.astype(jnp.int32), axis=1) - 1
    hit = mine[:, None, :] & (
        place[:, None, :] == jnp.arange(id_cap, dtype=jnp.int32)[None, :, None]
    )
    local_ids = jnp.sum(jnp.where(hit, all_ids[:, None, :] - seq_index * shard_rows, 0), axis=2)
    home = token_ids // shard_rows
    same = (home[None, :] == home[:, None]) & (
        jnp.arange(local_rows)[None, :] < jnp.arange(local_rows)[:, None]
    )
    arrive = home * id_cap + jnp.sum(same.astype(jnp.int32), axis=1)
    own = routes[:, 0]
    earlier = (own[None, :] == own[:, None]) & (
        jnp.arange(slot_rows)[None, :] < jnp.arange(slot_rows)[:, None]
    )
    slot_of = own * pair_cap + jnp.sum(earlier.astype(jnp.int32), axis=1)
    selector = (
        slot_of[None, :] == jnp.arange(seq_count * pair_cap, dtype=jnp.int32)[:, None]
    ).astype(jnp.bfloat16)
    counts = jnp.sum((all_routes == seq_index).astype(jnp.int32), axis=1)
    before = jnp.arange(seq_count)[None, :] < jnp.arange(seq_count)[:, None]
    offset = jnp.sum(jnp.where(before, counts[None, :], 0), axis=1)
    within = jnp.arange(pair_cap, dtype=jnp.int32)
    position = jnp.where(
        within[None, :] < counts[:, None],
        splice_start[0] + offset[:, None] + within[None, :],
        -1,
    ).reshape(-1)
    rows = jnp.arange(local_rows, dtype=jnp.int32)
    image = position[None, :] == rows[:, None]
    first = splice_start[0]
    is_image = (rows >= first) & (rows < first + jnp.sum(counts))
    text = (
        arrive[:, None] == jnp.arange(seq_count * id_cap, dtype=jnp.int32)[None, :]
    ) & ~is_image[:, None]
    return local_ids, selector, image.astype(jnp.bfloat16), text.astype(jnp.bfloat16)


def mega_kernel(
    vision_ref, gain_ref, w1_hbm, w2_hbm, text_ref, selector_ref, image_ref, placed_ref, out_ref,
    w1, w2, x_send, x_recv, half_send, half_recv, half_own, cross_send, cross_recv,
    h_send, h_recv, pair_send, pair_recv, pair_own, part_send, part_recv,
    row_send, row_recv, text_recv, total,
    w_sem, x_sems, half_sems, cross_sems, h_send_sems, h_recv_sems,
    pair_sems, part_sems, row_sems, text_sems,
):
    n, voc = lax.axis_size("seq"), lax.axis_size("vocab")
    s, v = lax.axis_index("seq"), lax.axis_index("vocab")
    chips = n // 2
    z, c = s // 2, s % 2
    split = n // voc
    f32, bf16 = jnp.float32, jnp.bfloat16
    slots = vision_ref.shape[0]

    def at(seq, vocab):
        return dict(device_id=(seq, vocab), device_id_type=pl.DeviceIdType.MESH)

    load1 = pltpu.make_async_copy(w1_hbm, w1, w_sem.at[0])
    load2 = pltpu.make_async_copy(w2_hbm, w2, w_sem.at[1])
    load1.start()
    load2.start()

    feeds = s // split
    barrier = pltpu.get_barrier_semaphore()
    for d in range(1, n):
        pl.semaphore_signal(barrier, inc=1, **at(lax.rem(s + d, n), v))
    for e in range(1, voc):
        for j in range(split):
            pl.semaphore_signal(barrier, inc=1, **at(v * split + j, lax.rem(v + e, voc)))

    @pl.when(feeds != v)
    def _():
        for r in range(n):
            pl.semaphore_signal(barrier, inc=1, **at(r, feeds))

    group = gain_ref.shape[1]
    depth = x_send.shape[2]
    for g in range(vision_ref.shape[1] // group):
        values = vision_ref[:, g * group : (g + 1) * group].astype(f32)
        center = values - jnp.mean(values, axis=-1, keepdims=True)
        spread = jnp.mean(center * center, axis=-1, keepdims=True)
        normed = (center / jnp.sqrt(spread + 1e-06) * gain_ref[...]).astype(bf16)
        for k in range(group // depth):
            x_send[g * (group // depth) + k] = normed[:, k * depth : (k + 1) * depth]

    pl.semaphore_wait(barrier, n - 1 + (voc - 1) * split + jnp.where(feeds != v, n, 0))

    def to_peer(source, target, sems, d, seq):
        copy = pltpu.make_async_remote_copy(
            src_ref=source,
            dst_ref=target,
            send_sem=sems.at[0, d],
            recv_sem=sems.at[1, d],
            **at(seq, v),
        )
        copy.start()
        return copy

    copies = []
    for d in range(1, n):
        peer = lax.rem(s + d, n)
        copies.append(to_peer(x_send.at[peer], x_recv.at[c, z], x_sems, d, peer))
    x_recv[c, z] = x_send[s]

    texts = []

    def send_text(ds):
        for d in ds:
            peer = lax.rem(s + d, n)
            texts.append(to_peer(text_ref.at[peer], text_recv.at[s], text_sems, d, peer))

    send_text(TEXT_A(n))
    text_recv[s] = text_ref[s]
    for copy in copies:
        copy.wait()

    def columns(width):
        return 256 if width % 256 == 0 else width

    def summed(lhs_ref, weight, to_sib, from_sib, own, send, recv, sems_pair, sems_part, ds):
        width = weight.shape[1]
        step = columns(width)
        rows = chips * slots
        for core, keep in ((1 - c, False), (c, True)):
            lhs = lhs_ref[core].reshape(rows, weight.shape[0])
            for k in range(0, width, step):
                part = jnp.dot(lhs, weight[:, k : k + step], preferred_element_type=f32)
                if keep:
                    own[:, k : k + step] = part
                else:
                    to_sib[:, k : k + step] = part.astype(bf16)
            if not keep:
                swap = to_peer(to_sib, from_sib, sems_pair, 0, s + 1 - 2 * c)
        swap.wait()
        sent = []
        for d in range(1, chips):
            other = lax.rem(z + d, chips)
            span = pl.ds(pl.multiple_of(other * slots, slots), slots)
            send[d] = (own[span, :] + from_sib[span, :].astype(f32)).astype(bf16)
            sent.append(to_peer(send.at[d], recv.at[d], sems_part, d, other * 2 + c))
        send_text(ds)
        span = pl.ds(pl.multiple_of(z * slots, slots), slots)
        value = own[span, :] + from_sib[span, :].astype(f32)
        for copy in sent:
            copy.wait()
        for d in range(1, chips):
            value = value + recv[d].astype(f32)
        return value

    load1.wait()
    pre = summed(x_recv, w1, half_send, half_recv, half_own, cross_send, cross_recv,
                 half_sems, cross_sems, TEXT_B(n))
    hidden = (0.5 * pre * (1.0 + lax.erf(pre * math.sqrt(0.5)))).astype(bf16)
    inner = h_send.shape[2]
    for j in range(split):
        h_send[j] = hidden[:, j * inner : (j + 1) * inner]

    def hidden_copy(e, j):
        return pltpu.make_async_remote_copy(
            src_ref=h_send.at[j],
            dst_ref=h_recv.at[c, z],
            send_sem=h_send_sems.at[e, j],
            recv_sem=h_recv_sems.at[s],
            **at(v * split + j, lax.rem(v + e, voc)),
        )

    for j in range(split):
        target = v * split + j

        @pl.when(target != s)
        def _():
            hidden_copy(0, j).start()

        @pl.when(target == s)
        def _():
            h_recv[c, z] = h_send[j]

        for e in range(1, voc):
            hidden_copy(e, j).start()
    send_text(TEXT_C(n))
    load2.wait()
    for r in range(n):
        def arrived():
            pltpu.make_async_remote_copy(
                src_ref=h_send.at[0],
                dst_ref=h_recv.at[r % 2, r // 2],
                send_sem=h_send_sems.at[0, 0],
                recv_sem=h_recv_sems.at[r],
                **at(lax.rem(s + 1, n), v),
            ).wait_recv()

        pl.when(jnp.logical_or(r != s, feeds != v))(arrived)

    merged = summed(h_recv, w2, pair_send, pair_recv, pair_own, part_send, part_recv,
                    pair_sems, part_sems, TEXT_D(n)).astype(bf16)

    width = w2.shape[1]
    cap = row_send.shape[1]
    outgoing = jnp.dot(selector_ref[...], merged, preferred_element_type=f32).astype(bf16)
    for t in range(n):
        row_send[t] = outgoing[t * cap : (t + 1) * cap]
    copies = []
    for d in range(1, n):
        peer = lax.rem(s + d, n)
        copies.append(to_peer(row_send.at[peer], row_recv.at[s], row_sems, d, peer))
    row_recv[s] = row_send[s]
    for copy in texts:
        copy.wait()
    step = columns(width)
    found = text_recv[...].reshape(-1, width)
    for k in range(0, width, step):
        total[:, k : k + step] = jnp.dot(
            placed_ref[...], found[:, k : k + step], preferred_element_type=f32
        )
    for copy in copies:
        copy.wait()
    for k in range(0, width, step):
        value = total[:, k : k + step]
        block = row_recv[:, :, k : k + step].astype(f32).reshape(n * cap, step).astype(bf16)
        value = value + jnp.dot(image_ref[...], block, preferred_element_type=f32)
        out_ref[:, k : k + step] = value.astype(bf16)
    for j in range(split):
        for e in range(voc):
            def left():
                hidden_copy(e, j).wait_send()

            if e == 0:
                pl.when(v * split + j != s)(left)
            else:
                left()


def TEXT_A(n):
    return range(1, 2)


def TEXT_B(n):
    return range(2, n // 2)


def TEXT_C(n):
    return range(n // 2, 3 * n // 4)


def TEXT_D(n):
    return range(3 * n // 4, n)


def mega(vision, gain, w1, w2, text, selector, image_pick, text_pick):
    n, voc = lax.axis_size("seq"), lax.axis_size("vocab")
    slots = vision.shape[0]
    rows = n // 2 * slots
    depth, mid = w1.shape
    inner, width = w2.shape
    cap = selector.shape[0] // n
    bf16, f32 = jnp.bfloat16, jnp.float32
    vmem = pl.BlockSpec(memory_space=pltpu.VMEM)
    hbm = pl.BlockSpec(memory_space=pl.ANY)
    dma = pltpu.SemaphoreType.DMA
    return pl.pallas_call(
        mega_kernel,
        out_shape=jax.ShapeDtypeStruct((image_pick.shape[0], width), bf16),
        in_specs=[vmem, vmem, hbm, hbm, vmem, vmem, vmem, vmem],
        out_specs=vmem,
        scratch_shapes=[
            pltpu.VMEM(w1.shape, bf16),
            pltpu.VMEM(w2.shape, bf16),
            pltpu.VMEM((n, slots, depth), bf16),
            pltpu.VMEM((2, n // 2, slots, depth), bf16),
            pltpu.VMEM((rows, mid), bf16),
            pltpu.VMEM((rows, mid), bf16),
            pltpu.VMEM((rows, mid), f32),
            pltpu.VMEM((n // 2, slots, mid), bf16),
            pltpu.VMEM((n // 2, slots, mid), bf16),
            pltpu.VMEM((n // voc, slots, inner), bf16),
            pltpu.VMEM((2, n // 2, slots, inner), bf16),
            pltpu.VMEM((rows, width), bf16),
            pltpu.VMEM((rows, width), bf16),
            pltpu.VMEM((rows, width), f32),
            pltpu.VMEM((n // 2, slots, width), bf16),
            pltpu.VMEM((n // 2, slots, width), bf16),
            pltpu.VMEM((n, cap, width), bf16),
            pltpu.VMEM((n, cap, width), bf16),
            pltpu.VMEM(text.shape, bf16),
            pltpu.VMEM((image_pick.shape[0], width), f32),
            dma((2,)),
            dma((2, n)),
            dma((2, 1)),
            dma((2, n // 2)),
            dma((voc, n // voc)),
            dma((n,)),
            dma((2, 1)),
            dma((2, n // 2)),
            dma((2, n)),
            dma((2, n)),
        ],
        compiler_params=pltpu.CompilerParams(
            collective_id=0, has_side_effects=True, vmem_limit_bytes=40 * 1024 * 1024
        ),
        name="merger",
    )(vision, gain[None, :], w1, w2, text, selector, image_pick, text_pick)


def on_device(token_ids, routes, splice_start, vision, ln_gain, table, w_fc1, w_fc2):
    local_ids, selector, image_pick, text_pick = route_plan(
        token_ids, routes, splice_start, table.shape[0]
    )
    text = gather_rows(local_ids, table)
    return mega(vision, ln_gain, w_fc1, w_fc2, text, selector, image_pick, text_pick)


def solution(mesh):
    in_specs = (
        P("seq"),
        P("seq", None),
        P("seq"),
        P("seq", None),
        P(),
        P("seq", "vocab"),
        P("seq", "vocab"),
        P("seq", "vocab"),
    )
    out_specs = P("seq", "vocab")
    return jax.shard_map(
        on_device, mesh=mesh, in_specs=in_specs, out_specs=out_specs, check_vma=False
    )
```
